32 devices in a mesh: node: 4 (over z), local: 8 (over y, x, core).
Axes of the slice: x: 2, y: 2, z: 4, core: 2. Of those that a mesh axis runs over, the one named last changes fastest.
Arguments:
- tokens: bfloat16 [4096, 5120], P(('node', 'local')), may hold values from -6 to 6
- routes: int32 [4096, 6], P(('node', 'local')), may hold values from 0 to 31, all different within a row; in each aligned block of 128 rows (0 to 127, 128 to 255, ...) at most 32 rows name the same one
- route_weights: float32 [4096, 6], P(('node', 'local')), may hold values from 0.05 to 1
- w_gate: bfloat16 [32, 5120, 768], P(('node', 'local')), may hold values from -0.078125 to 0.078125
- w_up: bfloat16 [32, 5120, 768], P(('node', 'local')), may hold values from -0.078125 to 0.078125
- w_down: bfloat16 [32, 768, 5120], P(('node', 'local')), may hold values from -0.21875 to 0.21875
Outputs:
- mixed: bfloat16 [4096, 5120], P(('node', 'local'))
- balance_loss: float32 [], replicated
The draws below stay inside these ranges and needn't reach their ends.
Inputs may be any that keep to these rules, and one draw needn't show every extreme that they name: `routes`: each row names 6 different experts. Among the rows of one device no expert is named more than 32 times, a bound that some block reaches.
All inputs are finite; a program needn't handle non-finite values.
Results may differ from the reference program's by a relative error of at most 0.0025.
The reference program's roundings to bfloat16 on the way count: a program that leaves them out, or rounds other values in their place, can miss the bound.
Values may be sent and summed in bfloat16 or wider, within the bound.
A program may use at most 128 MiB of HBM per device.

```python
import math
import jax
import jax.numpy as jnp
import numpy as np
from jax import lax

D = 5120
FF = 768
TOPK = 6
TOK_DEV = 128
EXPERTS = 32
TOKENS = 4096
CAP = 32
N_NODE = 4
N_LOCAL = 8


def block_scale(own_key, shape, split, least, largest):
    factor_of = 1.0
    for axis_at, shards_of in split:
        heights = jax.random.uniform(jax.random.fold_in(jax.random.fold_in(own_key, 6), axis_at), (shards_of,), jnp.float32, least / len(split), largest / len(split))
        factor_of = factor_of * jnp.repeat(jnp.exp(heights), shape[axis_at] // shards_of).reshape((-1,) + (1,) * (len(shape) - 1 - axis_at))
    return factor_of


def assign_block(key, own, number, rows, number_of, top, bound, skew):
    order = jax.random.permutation(key, number_of)
    crowded, ordinary = load_shares(number_of, rows * top, bound, skew, True), load_shares(number_of, rows * top, bound, skew, False)
    places = jnp.arange(number_of)

    def named(tallies, turn):
        used = int((tallies > 0).sum())
        fixed = max(1, used // 4)
        passed = fixed + (places - fixed + turn * (used - fixed)) % max(1, number_of - fixed)
        return jnp.zeros((number_of,), jnp.int32).at[order[jnp.where(places < fixed, places, passed)]].set(jnp.asarray(tallies, jnp.int32))

    tallies = jnp.where(number % 4 == 0, named(crowded, number // 4), named(ordinary, number - number // 4 - 1))
    mixed = jax.random.permutation(jax.random.fold_in(own, 3), number_of)
    giver, taker = mixed[0:number_of // 2 * 2:2], mixed[1:number_of // 2 * 2:2]
    room = jnp.minimum(tallies[giver] - 1, bound - tallies[taker]) // 2
    room = jnp.where((giver == order[0]) | (taker == order[0]) | (tallies[taker] == 0), 0, jnp.maximum(room, 0))
    passed = jax.random.randint(jax.random.fold_in(own, 4), (number_of // 2,), 0, 1 << 20) % (room + 1)
    tallies = tallies.at[giver].add(-passed).at[taker].add(passed)
    items = jnp.searchsorted(jnp.cumsum(tallies), jnp.arange(rows * top), side="right").astype(jnp.int32)
    table = items.reshape(top, rows).T
    table = table[jax.random.permutation(jax.random.fold_in(own, 1), rows)]
    turn = jax.random.randint(jax.random.fold_in(own, 2), (rows, 1), 0, top)
    return jnp.take_along_axis(table, (jnp.arange(top)[None, :] + turn) % top, axis=1)


def load_shares(number_of, total, bound, lean, full):
    portions = [(1 << 20) // math.isqrt(rank ** lean) + 1 for rank in range(1, number_of + 1)]
    largest = bound if full else min(bound, max(-(-total // number_of), total * portions[0] // sum(portions)))
    least = 1 if total - largest >= number_of - 1 else 0
    counts, surplus = [largest] + [least] * (number_of - 1), total - largest - least * (number_of - 1)
    while surplus > 0:
        free = [i for i in range(1, number_of) if counts[i] < largest] or [i for i in range(1, number_of) if counts[i] < bound]
        whole, remaining = sum([portions[i] for i in free]), surplus
        for i in free:
            more = min(bound - counts[i], max(1, remaining * portions[i] // whole), surplus)
            counts[i] = counts[i] + more
            surplus = surplus - more
    return np.array(counts)


def bell_draw(rng, shape, width, reach, split=(), kind=jnp.bfloat16):
    values = jax.random.normal(rng, shape, jnp.float32) * width
    if len(split) > 0:
        values = block_scale(rng, shape, split, -0.22, 0.18) * values
    return jnp.clip(values, min=-reach, max=reach).astype(kind)


def setup_inputs(seed: int = 0) -> dict:
    streams_of = jax.random.split(jax.random.key(seed), 7)
    tokens = bell_draw(streams_of[0], (TOKENS, D), 1.0, 6.0, ((0, 32),))
    routes_keys = jax.random.split(jax.random.fold_in(streams_of[1], 1), TOKENS // TOK_DEV)
    routes_turns = jax.random.permutation(jax.random.fold_in(streams_of[1], 3), TOKENS // TOK_DEV)
    routes = jax.vmap(lambda own, number: assign_block(jax.random.fold_in(streams_of[1], 2), own, number, TOK_DEV, EXPERTS, TOPK, CAP, 2))(routes_keys, routes_turns).reshape((TOKENS, TOPK))
    route_weights = jnp.clip(jnp.exp(math.log(1.0) - 2.9957323 * jax.random.uniform(streams_of[2], (TOKENS, TOPK), jnp.float32) ** block_scale(streams_of[2], (TOKENS, TOPK), ((0, 32),), -0.2, 0.2)), 0.05, 1.0)
    w_gate = bell_draw(streams_of[3], (EXPERTS, D, FF), D ** -0.5, 0.078125, ((0, 32),))
    w_up = bell_draw(streams_of[4], (EXPERTS, D, FF), D ** -0.5, 0.078125, ((0, 32),))
    w_down = bell_draw(streams_of[5], (EXPERTS, FF, D), FF ** -0.5, 0.21875, ((0, 32),))
    return {"tokens": tokens, "routes": routes, "route_weights": route_weights, "w_gate": w_gate, "w_up": w_up, "w_down": w_down}


def slots_of(flat):
    labels = jnp.arange(EXPERTS, dtype=jnp.int32)
    onehot = (flat[:, None] == labels[None, :]).astype(jnp.int32)
    running = jnp.cumsum(onehot, axis=0) - onehot
    return jnp.sum(running * onehot, axis=1).astype(jnp.int32)


def reference(tokens, routes, route_weights, w_gate, w_up, w_down):
    devices = N_NODE * N_LOCAL
    pairs = TOK_DEV * TOPK
    span = devices * CAP
    flat = routes.reshape(devices, pairs).astype(jnp.int32)
    slots = jax.vmap(slots_of)(flat)
    source = jnp.arange(devices, dtype=jnp.int32)[:, None]
    position = flat * span + source * CAP + slots
    token_ids = source * TOK_DEV + jnp.arange(pairs, dtype=jnp.int32)[None, :] // TOPK
    table = jnp.full((EXPERTS * span,), TOKENS, jnp.int32).at[position.reshape(-1)].set(token_ids.reshape(-1))
    padded = jnp.concatenate([tokens, jnp.zeros((1, D), jnp.bfloat16)], axis=0)

    def one_expert(packed):
        ids, gate_w, up_w, down_w = packed
        rows = padded[ids]
        gate = jnp.dot(rows, gate_w, preferred_element_type=jnp.float32)
        up = jnp.dot(rows, up_w, preferred_element_type=jnp.float32)
        hidden = (jax.nn.silu(gate) * up).astype(jnp.bfloat16)
        return jnp.dot(hidden, down_w, preferred_element_type=jnp.float32).astype(jnp.bfloat16)

    outputs = lax.map(one_expert, (table.reshape(EXPERTS, span), w_gate, w_up, w_down))
    outputs = outputs.reshape(EXPERTS * span, D)
    weights = route_weights.reshape(devices, TOK_DEV, TOPK)

    def one_source(packed):
        where, gates = packed
        picked = outputs[where].reshape(TOK_DEV, TOPK, D).astype(jnp.float32)
        return jnp.sum(gates[:, :, None] * picked, axis=1).astype(jnp.bfloat16)

    mixed = lax.map(one_source, (position, weights)).reshape(TOKENS, D)
    every = routes.reshape(-1).astype(jnp.int32)
    count = jax.ops.segment_sum(jnp.ones(every.shape, jnp.float32), every, num_segments=EXPERTS)
    weight_sum = jax.ops.segment_sum(route_weights.reshape(-1), every, num_segments=EXPERTS)
    total = jnp.float32(TOKENS)
    balance_loss = jnp.sum(count * weight_sum) * jnp.float32(EXPERTS) / (jnp.float32(TOPK) * total * total)
    return mixed, balance_loss
```

```python
import functools

import jax
import jax.numpy as jnp
from jax import lax
from jax.experimental import pallas as pl
from jax.experimental.pallas import tpu as pltpu
from jax.sharding import PartitionSpec as P

MESH = pl.DeviceIdType.MESH
VMEM_LIMIT = 62 * 1024 * 1024


def chunks_of(width):
    return max(n for n in range(1, 9) if width % (n * 128) == 0)


def greet(nn, nl, mn, ml):
    barrier = pltpu.get_barrier_semaphore()
    for k in range(1, nn):
        pl.semaphore_signal(barrier, inc=1, device_id={"node": lax.rem(mn + k, nn)}, device_id_type=MESH)
    for k in range(1, nl):
        pl.semaphore_signal(barrier, inc=1, device_id={"local": lax.rem(ml + k, nl)}, device_id_type=MESH)
    pl.semaphore_wait(barrier, nn + nl - 2)


def dispatch_kernel(nn, nl, nch, tok, pick, out, held, sent, z_send, z_recv, p_send, p_recv, own_sem):
    mn, ml = lax.axis_index("node"), lax.axis_index("local")
    tok_dev, width = tok.shape
    ch = width // nch
    rows = out.shape[1]
    mine = pl.ds(pl.multiple_of(mn * tok_dev, tok_dev), tok_dev)

    def cols(c):
        return pl.ds(pl.multiple_of(c * ch, 128), ch)

    def along(c, k):
        return pltpu.make_async_remote_copy(
            src_ref=tok.at[:, cols(c)],
            dst_ref=held.at[c, mine, :],
            send_sem=z_send.at[c, k - 1],
            recv_sem=z_recv.at[c, k - 1],
            device_id={"node": lax.rem(mn + k, nn)},
            device_id_type=MESH,
        )

    def block(e):
        return pl.ds(pl.multiple_of(e * rows, rows), rows)

    def within(c, k):
        e = lax.rem(ml + k, nl)
        return pltpu.make_async_remote_copy(
            src_ref=sent.at[c, block(e), :],
            dst_ref=out.at[ml, :, cols(c)],
            send_sem=p_send.at[c, k - 1],
            recv_sem=p_recv.at[c, k - 1],
            device_id={"local": e},
            device_id_type=MESH,
        )

    def own(c):
        return pltpu.make_async_copy(sent.at[c, block(ml), :], out.at[ml, :, cols(c)], own_sem.at[c])

    greet(nn, nl, mn, ml)

    @pl.loop(0, nch)
    def _(c):
        for k in range(1, nn):
            along(c, k).start()

    @pl.loop(0, nch)
    def _(c):
        held[c, mine, :] = tok[:, cols(c)]

    @pl.loop(0, nch)
    def _(c):
        for k in range(1, nn):
            along(c, k).wait_recv()
        picked = jnp.dot(pick[...], held[c], preferred_element_type=jnp.float32)
        sent[c] = picked.astype(jnp.bfloat16)
        for k in range(1, nl):
            within(c, k).start()
        own(c).start()

    @pl.loop(0, nch)
    def _(c):
        for k in range(1, nl):
            within(c, k).wait_recv()
        own(c).wait()
        for k in range(1, nn):
            along(c, k).wait_send()
        for k in range(1, nl):
            within(c, k).wait_send()


def return_kernel(nn, nl, nch, y, mix, out, held, part, got, p_send, p_recv, z_send, z_recv, own_sem):
    mn, ml = lax.axis_index("node"), lax.axis_index("local")
    tok_dev, width = out.shape
    ch = width // nch
    rows = y.shape[1]
    lines = nn * tok_dev
    mine = pl.ds(pl.multiple_of(ml * rows, rows), rows)

    def cols(c):
        return pl.ds(pl.multiple_of(c * ch, 128), ch)

    def within(c, k):
        e = lax.rem(ml + k, nl)
        return pltpu.make_async_remote_copy(
            src_ref=y.at[e, :, cols(c)],
            dst_ref=held.at[c, mine, :],
            send_sem=p_send.at[c, k - 1],
            recv_sem=p_recv.at[c, k - 1],
            device_id={"local": e},
            device_id_type=MESH,
        )

    def own(c):
        return pltpu.make_async_copy(y.at[ml, :, cols(c)], held.at[c, mine, :], own_sem.at[c])

    def tokens_of(p):
        return pl.ds(pl.multiple_of(p * tok_dev, tok_dev), tok_dev)

    def along(c, k):
        p = lax.rem(mn + k, nn)
        return pltpu.make_async_remote_copy(
            src_ref=part.at[c, tokens_of(p), :],
            dst_ref=got.at[c, k - 1],
            send_sem=z_send.at[c, k - 1],
            recv_sem=z_recv.at[c, k - 1],
            device_id={"node": p},
            device_id_type=MESH,
        )

    greet(nn, nl, mn, ml)

    @pl.loop(0, nch)
    def _(c):
        for k in range(1, nl):
            within(c, k).start()
        own(c).start()

    @pl.loop(0, nch)
    def _(c):
        for k in range(1, nl):
            within(c, k).wait_recv()
        own(c).wait()
        terms = [
            jnp.dot(mix[pl.ds(i * lines, lines), :], held[c], preferred_element_type=jnp.float32)
            for i in range(3)
        ]
        part[c] = terms[0] + terms[1] + terms[2]
        for k in range(1, nn):
            along(c, k).start()

    @pl.loop(0, nch)
    def _(c):
        total = part[c, tokens_of(mn), :]
        for k in range(1, nn):
            along(c, k).wait_recv()
        for k in range(1, nn):
            total = total + got[c, k - 1]
        out[:, cols(c)] = total.astype(out.dtype)
        for k in range(1, nl):
            within(c, k).wait_send()
        for k in range(1, nn):
            along(c, k).wait_send()


def sems(*shape):
    return pltpu.SemaphoreType.DMA(shape)


def local(tokens, routes, route_weights, w_gate, w_up, w_down):
    nn, nl = lax.axis_size("node"), lax.axis_size("local")
    mn, ml = lax.axis_index("node"), lax.axis_index("local")
    devices = nn * nl
    exp_dev = w_gate.shape[0]
    experts = exp_dev * devices
    assert exp_dev == 1
    tok_dev, width = tokens.shape
    topk = routes.shape[1]
    cap = 4 * tok_dev * topk // (3 * experts)
    rows = nn * cap
    nch = chunks_of(width)
    ch = width // nch
    f32, bf16 = jnp.float32, jnp.bfloat16

    both = jnp.concatenate([routes.astype(f32), route_weights], axis=1)
    every = lax.all_gather(both, ("node", "local"), axis=0, tiled=True)
    every_routes = every[:, :topk].astype(jnp.int32)
    labels = jnp.arange(experts, dtype=jnp.int32)
    hit = every_routes[:, :, None] == labels[None, None, :]
    counts = jnp.sum(hit.astype(f32), axis=(0, 1))
    sums = jnp.sum(jnp.where(hit, every[:, topk:, None], 0.0), axis=(0, 1))
    total = jnp.float32(tok_dev * devices)
    balance_loss = jnp.sum(counts * sums) * jnp.float32(experts) / (jnp.float32(topk) * total * total)

    line = lax.dynamic_index_in_dim(every.reshape(nn, nl, tok_dev, 2 * topk), ml, 1, keepdims=False)
    plane = mn * nl + jnp.arange(nl, dtype=jnp.int32)
    chosen = line[..., :topk, None].astype(jnp.int32) == plane
    named = jnp.any(chosen, axis=2)
    weight = jnp.sum(jnp.where(chosen, line[..., topk:, None], 0.0), axis=2)
    before = jnp.tril(jnp.ones((tok_dev, tok_dev), bf16), -1)
    slot = jnp.einsum("ut,pte->pue", before, named.astype(bf16), preferred_element_type=f32)
    slot = jnp.where(named, slot.astype(jnp.int32), -1)
    where = (
        (slot.transpose(2, 0, 1)[:, None, None] == jnp.arange(cap)[None, None, :, None, None])
        & (jnp.arange(nn)[:, None] == jnp.arange(nn)[None, :])[None, :, None, :, None]
    )
    pick = where.astype(bf16).reshape(nl * rows, nn * tok_dev)
    back = (
        (slot[:, :, :, None, None] == jnp.arange(cap)[None, None, None, None, :])
        & (jnp.arange(nn)[:, None] == jnp.arange(nn)[None, :])[:, None, None, :, None]
    )
    high = lax.reduce_precision(weight, 8, 7)
    middle = lax.reduce_precision(weight - high, 8, 7)
    low = lax.reduce_precision(weight - high - middle, 8, 7)
    mix = jnp.where(back[None], jnp.stack([high, middle, low])[..., None, None], 0.0).astype(bf16)
    mix = mix.reshape(3 * nn * tok_dev, nl * rows)

    vmem = pl.BlockSpec(memory_space=pltpu.VMEM)
    hbm = pl.BlockSpec(memory_space=pl.ANY)
    got = pl.pallas_call(
        functools.partial(dispatch_kernel, nn, nl, nch),
        out_shape=jax.ShapeDtypeStruct((nl, rows, width), bf16),
        in_specs=[vmem, vmem],
        out_specs=hbm,
        scratch_shapes=[
            pltpu.VMEM((nch, nn * tok_dev, ch), bf16),
            pltpu.VMEM((nch, nl * rows, ch), bf16),
            sems(nch, nn - 1),
            sems(nch, nn - 1),
            sems(nch, nl - 1),
            sems(nch, nl - 1),
            sems(nch),
        ],
        compiler_params=pltpu.CompilerParams(
            collective_id=0, has_side_effects=True, vmem_limit_bytes=VMEM_LIMIT
        ),
    )(tokens, pick)
    got = got.reshape(nl * rows, width)
    gate = jnp.dot(got, w_gate[0], preferred_element_type=f32)
    upper = jnp.dot(got, w_up[0], preferred_element_type=f32)
    hidden = (jax.nn.silu(gate) * upper).astype(bf16)
    y = jnp.dot(hidden, w_down[0], preferred_element_type=f32).astype(bf16)

    mixed = pl.pallas_call(
        functools.partial(return_kernel, nn, nl, nch),
        out_shape=jax.ShapeDtypeStruct((tok_dev, width), bf16),
        in_specs=[hbm, vmem],
        out_specs=vmem,
        scratch_shapes=[
            pltpu.VMEM((nch, nl * rows, ch), bf16),
            pltpu.VMEM((nch, nn * tok_dev, ch), f32),
            pltpu.VMEM((nch, nn - 1, tok_dev, ch), f32),
            sems(nch, nl - 1),
            sems(nch, nl - 1),
            sems(nch, nn - 1),
            sems(nch, nn - 1),
            sems(nch),
        ],
        compiler_params=pltpu.CompilerParams(
            collective_id=1, has_side_effects=True, vmem_limit_bytes=VMEM_LIMIT
        ),
    )(y.reshape(nl, rows, width), mix)
    return (mixed, balance_loss)


def solution(mesh):
    placed = (
        P(("node", "local"), None),
        P(("node", "local"), None),
        P(("node", "local"), None),
        P(("node", "local"), None, None),
        P(("node", "local"), None, None),
        P(("node", "local"), None, None),
    )
    return jax.shard_map(
        local,
        mesh=mesh,
        in_specs=placed,
        out_specs=(P(("node", "local"), None), P()),
        check_vma=False,
    )
```

```python
import functools

import jax
import jax.numpy as jnp
from jax import lax
from jax.experimental import pallas as pl
from jax.experimental.pallas import tpu as pltpu
from jax.sharding import PartitionSpec as P

MESH = pl.DeviceIdType.MESH
VMEM_LIMIT = 62 * 1024 * 1024


def chunks_of(width):
    return max(n for n in range(1, 11) if width % (n * 128) == 0)


def greet(nn, nl, mn, ml):
    barrier = pltpu.get_barrier_semaphore()
    for k in range(1, nn):
        pl.semaphore_signal(barrier, inc=1, device_id={"node": lax.rem(mn + k, nn)}, device_id_type=MESH)
    for k in range(1, nl):
        pl.semaphore_signal(barrier, inc=1, device_id={"local": lax.rem(ml + k, nl)}, device_id_type=MESH)
    pl.semaphore_wait(barrier, nn + nl - 2)


def dispatch_kernel(nn, nl, nch, tok, pick, out, held, sent, z_send, z_recv, p_send, p_recv, own_sem):
    mn, ml = lax.axis_index("node"), lax.axis_index("local")
    tok_dev, width = tok.shape
    ch = width // nch
    rows = out.shape[1]
    mine = pl.ds(pl.multiple_of(mn * tok_dev, tok_dev), tok_dev)

    def cols(c):
        return pl.ds(pl.multiple_of(c * ch, 128), ch)

    def along(c, k):
        return pltpu.make_async_remote_copy(
            src_ref=tok.at[:, cols(c)],
            dst_ref=held.at[c, mine, :],
            send_sem=z_send.at[c, k - 1],
            recv_sem=z_recv.at[c, k - 1],
            device_id={"node": lax.rem(mn + k, nn)},
            device_id_type=MESH,
        )

    def block(e):
        return pl.ds(pl.multiple_of(e * rows, rows), rows)

    def within(c, k):
        e = lax.rem(ml + k, nl)
        return pltpu.make_async_remote_copy(
            src_ref=sent.at[c, block(e), :],
            dst_ref=out.at[ml, :, cols(c)],
            send_sem=p_send.at[c, k - 1],
            recv_sem=p_recv.at[c, k - 1],
            device_id={"local": e},
            device_id_type=MESH,
        )

    def own(c):
        return pltpu.make_async_copy(sent.at[c, block(ml), :], out.at[ml, :, cols(c)], own_sem.at[c])

    greet(nn, nl, mn, ml)

    @pl.loop(0, nch)
    def _(c):
        for k in range(1, nn):
            along(c, k).start()

    @pl.loop(0, nch)
    def _(c):
        held[c, mine, :] = tok[:, cols(c)]

    @pl.loop(0, nch)
    def _(c):
        for k in range(1, nn):
            along(c, k).wait_recv()
        picked = jnp.dot(pick[...], held[c], preferred_element_type=jnp.float32)
        sent[c] = picked.astype(jnp.bfloat16)
        for k in range(1, nl):
            within(c, k).start()
        own(c).start()

    @pl.loop(0, nch)
    def _(c):
        for k in range(1, nl):
            within(c, k).wait_recv()
        own(c).wait()
        for k in range(1, nn):
            along(c, k).wait_send()
        for k in range(1, nl):
            within(c, k).wait_send()


def return_kernel(nn, nl, nch, y, mix, out, held, part, got, p_send, p_recv, z_send, z_recv, own_sem):
    mn, ml = lax.axis_index("node"), lax.axis_index("local")
    tok_dev, width = out.shape
    ch = width // nch
    rows = y.shape[1]
    lines = nn * tok_dev
    mine = pl.ds(pl.multiple_of(ml * rows, rows), rows)

    def cols(c):
        return pl.ds(pl.multiple_of(c * ch, 128), ch)

    def within(c, k):
        e = lax.rem(ml + k, nl)
        return pltpu.make_async_remote_copy(
            src_ref=y.at[e, :, cols(c)],
            dst_ref=held.at[c, mine, :],
            send_sem=p_send.at[c, k - 1],
            recv_sem=p_recv.at[c, k - 1],
            device_id={"local": e},
            device_id_type=MESH,
        )

    def own(c):
        return pltpu.make_async_copy(y.at[ml, :, cols(c)], held.at[c, mine, :], own_sem.at[c])

    def tokens_of(p):
        return pl.ds(pl.multiple_of(p * tok_dev, tok_dev), tok_dev)

    def along(c, k):
        p = lax.rem(mn + k, nn)
        return pltpu.make_async_remote_copy(
            src_ref=part.at[c, tokens_of(p), :],
            dst_ref=got.at[c, k - 1],
            send_sem=z_send.at[c, k - 1],
            recv_sem=z_recv.at[c, k - 1],
            device_id={"node": p},
            device_id_type=MESH,
        )

    greet(nn, nl, mn, ml)

    @pl.loop(0, nch)
    def _(c):
        for k in range(1, nl):
            within(c, k).start()
        own(c).start()

    @pl.loop(0, nch)
    def _(c):
        for k in range(1, nl):
            within(c, k).wait_recv()
        own(c).wait()
        terms = [
            jnp.dot(mix[pl.ds(i * lines, lines), :], held[c], preferred_element_type=jnp.float32)
            for i in range(3)
        ]
        part[c] = terms[0] + terms[1] + terms[2]
        for k in range(1, nn):
            along(c, k).start()

    @pl.loop(0, nch)
    def _(c):
        total = part[c, tokens_of(mn), :]
        for k in range(1, nn):
            along(c, k).wait_recv()
        for k in range(1, nn):
            total = total + got[c, k - 1]
        out[:, cols(c)] = total.astype(out.dtype)
        for k in range(1, nl):
            within(c, k).wait_send()
        for k in range(1, nn):
            along(c, k).wait_send()


def sems(*shape):
    return pltpu.SemaphoreType.DMA(shape)


def local(tokens, routes, route_weights, w_gate, w_up, w_down):
    nn, nl = lax.axis_size("node"), lax.axis_size("local")
    mn, ml = lax.axis_index("node"), lax.axis_index("local")
    devices = nn * nl
    exp_dev = w_gate.shape[0]
    experts = exp_dev * devices
    assert exp_dev == 1
    tok_dev, width = tokens.shape
    topk = routes.shape[1]
    cap = 4 * tok_dev * topk // (3 * experts)
    rows = nn * cap
    nch = chunks_of(width)
    ch = width // nch
    f32, bf16 = jnp.float32, jnp.bfloat16

    both = jnp.concatenate([routes.astype(f32), route_weights], axis=1)
    every = lax.all_gather(both, ("node", "local"), axis=0, tiled=True)
    every_routes = every[:, :topk].astype(jnp.int32)
    labels = jnp.arange(experts, dtype=jnp.int32)
    hit = every_routes[:, :, None] == labels[None, None, :]
    counts = jnp.sum(hit.astype(f32), axis=(0, 1))
    sums = jnp.sum(jnp.where(hit, every[:, topk:, None], 0.0), axis=(0, 1))
    total = jnp.float32(tok_dev * devices)
    balance_loss = jnp.sum(counts * sums) * jnp.float32(experts) / (jnp.float32(topk) * total * total)

    line = lax.dynamic_index_in_dim(every.reshape(nn, nl, tok_dev, 2 * topk), ml, 1, keepdims=False)
    plane = mn * nl + jnp.arange(nl, dtype=jnp.int32)
    chosen = line[..., :topk, None].astype(jnp.int32) == plane
    named = jnp.any(chosen, axis=2)
    weight = jnp.sum(jnp.where(chosen, line[..., topk:, None], 0.0), axis=2)
    before = jnp.tril(jnp.ones((tok_dev, tok_dev), bf16), -1)
    slot = jnp.einsum("ut,pte->pue", before, named.astype(bf16), preferred_element_type=f32)
    slot = jnp.where(named, slot.astype(jnp.int32), -1)
    where = (
        (slot.transpose(2, 0, 1)[:, None, None] == jnp.arange(cap)[None, None, :, None, None])
        & (jnp.arange(nn)[:, None] == jnp.arange(nn)[None, :])[None, :, None, :, None]
    )
    pick = where.astype(bf16).reshape(nl * rows, nn * tok_dev)
    back = (
        (slot[:, :, :, None, None] == jnp.arange(cap)[None, None, None, None, :])
        & (jnp.arange(nn)[:, None] == jnp.arange(nn)[None, :])[:, None, None, :, None]
    )
    high = lax.reduce_precision(weight, 8, 7)
    middle = lax.reduce_precision(weight - high, 8, 7)
    low = lax.reduce_precision(weight - high - middle, 8, 7)
    mix = jnp.where(back[None], jnp.stack([high, middle, low])[..., None, None], 0.0).astype(bf16)
    mix = mix.reshape(3 * nn * tok_dev, nl * rows)

    vmem = pl.BlockSpec(memory_space=pltpu.VMEM)
    hbm = pl.BlockSpec(memory_space=pl.ANY)
    got = pl.pallas_call(
        functools.partial(dispatch_kernel, nn, nl, nch),
        out_shape=jax.ShapeDtypeStruct((nl, rows, width), bf16),
        in_specs=[vmem, vmem],
        out_specs=hbm,
        scratch_shapes=[
            pltpu.VMEM((nch, nn * tok_dev, ch), bf16),
            pltpu.VMEM((nch, nl * rows, ch), bf16),
            sems(nch, nn - 1),
            sems(nch, nn - 1),
            sems(nch, nl - 1),
            sems(nch, nl - 1),
            sems(nch),
        ],
        compiler_params=pltpu.CompilerParams(
            collective_id=0, has_side_effects=True, vmem_limit_bytes=VMEM_LIMIT
        ),
    )(tokens, pick)
    got = got.reshape(nl * rows, width)
    gate = jnp.dot(got, w_gate[0], preferred_element_type=f32)
    upper = jnp.dot(got, w_up[0], preferred_element_type=f32)
    hidden = (jax.nn.silu(gate) * upper).astype(bf16)
    y = jnp.dot(hidden, w_down[0], preferred_element_type=f32).astype(bf16)

    mixed = pl.pallas_call(
        functools.partial(return_kernel, nn, nl, nch),
        out_shape=jax.ShapeDtypeStruct((tok_dev, width), bf16),
        in_specs=[hbm, vmem],
        out_specs=vmem,
        scratch_shapes=[
            pltpu.VMEM((nch, nl * rows, ch), bf16),
            pltpu.VMEM((nch, nn * tok_dev, ch), f32),
            pltpu.VMEM((nch, nn - 1, tok_dev, ch), f32),
            sems(nch, nl - 1),
            sems(nch, nl - 1),
            sems(nch, nn - 1),
            sems(nch, nn - 1),
            sems(nch),
        ],
        compiler_params=pltpu.CompilerParams(
            collective_id=1, has_side_effects=True, vmem_limit_bytes=VMEM_LIMIT
        ),
    )(y.reshape(nl, rows, width), mix)
    return (mixed, balance_loss)


def solution(mesh):
    placed = (
        P(("node", "local"), None),
        P(("node", "local"), None),
        P(("node", "local"), None),
        P(("node", "local"), None, None),
        P(("node", "local"), None, None),
        P(("node", "local"), None, None),
    )
    return jax.shard_map(
        local,
        mesh=mesh,
        in_specs=placed,
        out_specs=(P(("node", "local"), None), P()),
        check_vma=False,
    )
```
